1024 devices in a mesh: ex: 8 (over x, y_lo), ey: 4 (over y_hi), tp: 32 (over z, core).
Axes of the slice: x: 4, y: 8 (y_hi: 4, y_lo: 2; y = y_hi * 2 + y_lo), z: 16, core: 2. Of those that a mesh axis runs over, the one named last changes fastest.
Arguments:
- tokens: bfloat16 [1024, 7168], P(('ex', 'ey'), 'tp'), may hold values from -6 to 6
- cotangent: bfloat16 [1024, 7168], P(('ex', 'ey'), 'tp'), may hold values from -0.59765625 to 0.59765625
- gates: bfloat16 [1024, 8], P(('ex', 'ey')), may hold values from 0.049804688 to 1
- expert_ids: int32 [1024, 8], P(('ex', 'ey')), may hold values from 0 to 31, all different within a row; in each aligned block of 32 rows (0 to 31, 32 to 63, ...) at most 10 rows name the same one
- saved_gate: bfloat16 [1024, 32, 320], P(None, ('ex', 'ey')), may hold values from -6 to 6
- saved_up: bfloat16 [1024, 32, 320], P(None, ('ex', 'ey')), may hold values from -6 to 6
- w_gate: bfloat16 [32, 7168, 1024], P(('ex', 'ey'), 'tp'), may hold values from -0.1875 to 0.1875
- w_up: bfloat16 [32, 7168, 1024], P(('ex', 'ey'), 'tp'), may hold values from -0.1875 to 0.1875
- w_down: bfloat16 [32, 1024, 7168], P(('ex', 'ey'), None, 'tp'), may hold values from -0.375 to 0.375
Outputs:
- grad_tokens: bfloat16 [1024, 7168], P(('ex', 'ey'), 'tp')
- grad_gates: bfloat16 [1024, 8], P(('ex', 'ey'))
- grad_w_gate: bfloat16 [32, 7168, 1024], P(('ex', 'ey'), 'tp')
- grad_w_up: bfloat16 [32, 7168, 1024], P(('ex', 'ey'), 'tp')
- grad_w_down: bfloat16 [32, 1024, 7168], P(('ex', 'ey'), None, 'tp')
The draws below stay inside these ranges and needn't reach their ends.
Inputs may be any that keep to these rules, and one draw needn't show every extreme that they name: `expert_ids`: each row names 8 different experts. The rows of one token group name any one expert at most 10 times, a bound that some block reaches.
All inputs are finite; a program needn't handle non-finite values.
Results may differ from the reference program's by a relative error of at most 0.025.
Values may be sent and summed in bfloat16 or wider, within the bound.
No kernel may reach another device: no remote copies, remote signals or barrier semaphores. Data moves between devices by JAX's collectives and lax.ppermute only.
A program may use at most 32 MiB of HBM per device.

```python
import math
import jax
import jax.numpy as jnp
import numpy as np
from jax import lax

D = 7168
FF = 1024
EXPERTS = 32
TOP = 8
TOK_DEV = 32
CAP = 10
SLOTS = 320
TOKENS = 1024
N_EX = 8
N_EY = 4
N_TP = 32


def spiked(entries, rng, source, target, blocks, factor):
    owner, partner = [(jnp.arange(entries.shape[dim]) // (entries.shape[dim] // blocks)).reshape([-1 if axis == dim else 1 for axis in range(entries.ndim)]) for dim in (source, target)]
    chosen = jax.random.permutation(rng, blocks)[partner]
    strong = (owner == chosen) | (owner == (partner + blocks // 2) % blocks)
    return jnp.where(strong, factor * entries, entries)


def levels(stream_key, shape, shards, low, high):
    gain, own = 1.0, jax.random.fold_in(stream_key, 6)
    for dim, parts in shards:
        draws = jnp.exp(jax.random.uniform(jax.random.fold_in(own, dim), (parts,), jnp.float32, low / len(shards), high / len(shards)))
        gain = gain * jnp.repeat(draws, shape[dim] // parts).reshape([-1 if axis == dim else 1 for axis in range(len(shape))])
    return gain


def assign_block(own_key, own, number, rows, count, top, most, skew):
    ranking = jax.random.permutation(own_key, count)
    heavy_load, usual = shares(count, rows * top, most, skew, True), shares(count, rows * top, most, skew, False)
    places = jnp.arange(count)

    def named(lengths, rotation):
        used = int((lengths > 0).sum())
        fixed = max(1, used // 4)
        moved = fixed + (places - fixed + rotation * (used - fixed)) % max(1, count - fixed)
        return jnp.zeros((count,), jnp.int32).at[ranking[jnp.where(places < fixed, places, moved)]].set(jnp.asarray(lengths, jnp.int32))

    lengths = jnp.where(number % 4 == 0, named(heavy_load, number // 4), named(usual, number - number // 4 - 1))
    mixed = jax.random.permutation(jax.random.fold_in(own, 3), count)
    donor, receiver = mixed[0:count // 2 * 2:2], mixed[1:count // 2 * 2:2]
    room = jnp.minimum(lengths[donor] - 1, most - lengths[receiver]) // 2
    room = jnp.where((donor == ranking[0]) | (receiver == ranking[0]) | (lengths[receiver] == 0), 0, jnp.maximum(room, 0))
    moved = jax.random.randint(jax.random.fold_in(own, 4), (count // 2,), 0, 1 << 20) % (room + 1)
    lengths = lengths.at[donor].add(-moved).at[receiver].add(moved)
    labels = jnp.searchsorted(jnp.cumsum(lengths), jnp.arange(rows * top), side="right").astype(jnp.int32)
    table = labels.reshape(top, rows).T
    table = table[jax.random.permutation(jax.random.fold_in(own, 1), rows)]
    rotation = jax.random.randint(jax.random.fold_in(own, 2), (rows, 1), 0, top)
    return jnp.take_along_axis(table, (jnp.arange(top)[None, :] + rotation) % top, axis=1)


def shares(count, total, most, skew, full):
    weights = [(1 << 20) // math.isqrt(standing ** skew) + 1 for standing in range(1, count + 1)]
    largest = most if full else min(most, max(-(-total // count), total * weights[0] // sum(weights)))
    least = 1 if total - largest >= count - 1 else 0
    holding, spare = [largest] + [least] * (count - 1), total - largest - least * (count - 1)
    while spare > 0:
        candidates = [i for i in range(1, count) if holding[i] < largest] or [i for i in range(1, count) if holding[i] < most]
        mass, budget = sum([weights[i] for i in candidates]), spare
        for i in candidates:
            addition = min(most - holding[i], max(1, budget * weights[i] // mass), spare)
            holding[i] = holding[i] + addition
            spare = spare - addition
    return np.array(holding)


def centred(stream_key, shape, deviation, limit, shards=(), kind=jnp.bfloat16):
    entries = jax.random.normal(stream_key, shape, jnp.float32) * deviation
    if len(shards) > 0:
        entries = levels(stream_key, shape, shards, -0.22, 0.18) * entries
    return jnp.clip(entries, min=-limit, max=limit).astype(kind)


def heavy_noise(key, shape, scale, limit, cuts, heavy, held_as=jnp.bfloat16):
    result = scale * jax.random.normal(key, shape, jnp.float32)
    if cuts:
        result = result * levels(key, shape, cuts, -0.22, 0.18)
    return jnp.clip(spiked(result, jax.random.fold_in(key, 3), *heavy), -limit, limit).astype(held_as)


def setup_inputs(seed: int = 0) -> dict:
    splits = jax.random.split(jax.random.key(seed), 10)
    tokens = centred(splits[0], (TOKENS, D), 1.0, 6.0, ((0, 32), (1, 32)))
    cotangent = centred(splits[1], (TOKENS, D), 0.1, 0.59765625, ((0, 32), (1, 32)))
    gates = jnp.clip(jnp.exp(math.log(1.0) - 2.9996462 * jax.random.uniform(splits[2], (TOKENS, TOP), jnp.float32) ** levels(splits[2], (TOKENS, TOP), ((0, 32),), -0.2, 0.2)), 0.049804688, 1.0).astype(jnp.bfloat16)
    expert_ids_keys = jax.random.split(jax.random.fold_in(splits[3], 1), TOKENS // TOK_DEV)
    expert_ids_turns = jax.random.permutation(jax.random.fold_in(splits[3], 3), TOKENS // TOK_DEV)
    expert_ids = jax.vmap(lambda own, number: assign_block(jax.random.fold_in(splits[3], 2), own, number, TOK_DEV, EXPERTS, TOP, CAP, 0))(expert_ids_keys, expert_ids_turns).reshape((TOKENS, TOP))
    saved_gate = centred(splits[4], (FF, EXPERTS, SLOTS), 1.0, 6.0, ((1, 32),))
    saved_up = centred(splits[5], (FF, EXPERTS, SLOTS), 1.0, 6.0, ((1, 32),))
    w_gate = centred(splits[6], (EXPERTS, D, FF), FF ** -0.5, 0.1875, ((0, 32), (1, 32)))
    w_up = centred(splits[7], (EXPERTS, D, FF), FF ** -0.5, 0.1875, ((0, 32), (1, 32)))
    w_down = heavy_noise(splits[8], (EXPERTS, FF, D), FF ** -0.5, 0.375, ((0, 32), (2, 32)), (2, 1, 32, 2.75))
    return {"tokens": tokens, "cotangent": cotangent, "gates": gates, "expert_ids": expert_ids, "saved_gate": saved_gate, "saved_up": saved_up, "w_gate": w_gate, "w_up": w_up, "w_down": w_down}


def slot_codes(expert_ids, capacity, expert_count):
    tok_rows, top_count = expert_ids.shape
    flat = expert_ids.reshape(-1)
    onehot = (flat[:, None] == jnp.arange(expert_count, dtype=jnp.int32)[None, :]).astype(jnp.int32)
    before = jnp.cumsum(onehot, axis=0) - onehot
    position = jnp.sum(before * onehot, axis=1)
    return (flat * capacity + position).reshape(tok_rows, top_count)


def reference(tokens, cotangent, gates, expert_ids, saved_gate, saved_up, w_gate, w_up, w_down):
    source_count = N_EX * N_EY
    slot_total = source_count * CAP
    block_width = D // N_TP
    blocks = expert_ids.reshape(source_count, TOK_DEV, TOP)
    codes = jax.vmap(lambda stretch_ids: slot_codes(stretch_ids, CAP, EXPERTS))(blocks)
    position = codes - blocks * CAP
    source = jnp.arange(source_count, dtype=jnp.int32)[:, None, None]
    row_id = (blocks * slot_total + source * CAP + position).reshape(TOKENS, TOP).astype(jnp.int32)
    pair_index = jnp.arange(TOKENS * TOP, dtype=jnp.int32)
    table = jnp.full((EXPERTS * slot_total,), TOKENS * TOP, jnp.int32).at[row_id.reshape(-1)].set(pair_index)
    table = table.reshape(EXPERTS, slot_total)
    x_pad = jnp.concatenate([tokens, jnp.zeros((1, D), tokens.dtype)], axis=0)
    dy_pad = jnp.concatenate([cotangent, jnp.zeros((1, D), cotangent.dtype)], axis=0)
    g_pad = jnp.concatenate([gates.reshape(-1), jnp.zeros((1,), gates.dtype)], axis=0)
    gate_major = jnp.moveaxis(saved_gate, 1, 0)
    up_major = jnp.moveaxis(saved_up, 1, 0)

    def one_expert(bundle):
        pairs, weight_gate, weight_up, weight_down, gate_pre, up_pre = bundle
        token_row = pairs // TOP
        x_rows = x_pad[token_row]
        dy_rows = dy_pad[token_row]
        g_rows = g_pad[pairs]
        scaled = (g_rows.astype(jnp.float32)[:, None] * dy_rows.astype(jnp.float32)).astype(jnp.bfloat16)
        act_gate = gate_pre.astype(jnp.float32)
        act_up = up_pre.astype(jnp.float32)
        sigm = jax.nn.sigmoid(act_gate)
        hidden = (act_gate * sigm * act_up).astype(jnp.bfloat16)
        out_rows = lax.dot_general(hidden, weight_down, (((0,), (0,)), ((), ())), preferred_element_type=jnp.float32)
        prod = (dy_rows.astype(jnp.float32) * out_rows).reshape(slot_total, N_TP, block_width)
        score_part = lax.optimization_barrier(jnp.sum(prod, axis=2).astype(jnp.bfloat16))
        score = jnp.sum(score_part.astype(jnp.float32), axis=1).astype(jnp.bfloat16)
        down_blocks = weight_down.astype(jnp.float32).reshape(FF, N_TP, block_width)
        scaled_blocks = scaled.astype(jnp.float32).reshape(slot_total, N_TP, block_width)
        dh_part = jnp.einsum("fjd,sjd->jfs", down_blocks, scaled_blocks, precision=lax.Precision.HIGHEST)
        dh_part = lax.optimization_barrier(dh_part.astype(jnp.bfloat16))
        dh_sum = jnp.sum(dh_part.astype(jnp.float32), axis=0).astype(jnp.bfloat16)
        dh_wide = dh_sum.astype(jnp.float32)
        d_gate_pre = (dh_wide * act_up * sigm * (1.0 + act_gate * (1.0 - sigm))).astype(jnp.bfloat16)
        d_up_pre = (dh_wide * act_gate * sigm).astype(jnp.bfloat16)
        dims = (((0,), (1,)), ((), ()))
        dx_rows = lax.dot_general(d_gate_pre, weight_gate, dims, preferred_element_type=jnp.float32)
        dx_rows = dx_rows + lax.dot_general(d_up_pre, weight_up, dims, preferred_element_type=jnp.float32)
        grad_gate_w = lax.dot_general(x_rows, d_gate_pre, dims, preferred_element_type=jnp.float32)
        grad_up_w = lax.dot_general(x_rows, d_up_pre, dims, preferred_element_type=jnp.float32)
        grad_down_w = jnp.dot(hidden, scaled, preferred_element_type=jnp.float32)
        return (dx_rows.astype(jnp.bfloat16), score, grad_gate_w.astype(jnp.bfloat16),
                grad_up_w.astype(jnp.bfloat16), grad_down_w.astype(jnp.bfloat16))

    dx_all, score_all, grad_w_gate, grad_w_up, grad_w_down = lax.map(
        one_expert, (table, w_gate, w_up, w_down, gate_major, up_major))
    dx_flat = dx_all.reshape(EXPERTS * slot_total, D)
    total = jnp.zeros((TOKENS, D), jnp.float32)
    for choice_index in range(TOP):
        total = total + dx_flat[row_id[:, choice_index]].astype(jnp.float32)
    grad_tokens = total.astype(jnp.bfloat16)
    grad_gates = score_all.reshape(-1)[row_id]
    return grad_tokens, grad_gates, grad_w_gate, grad_w_up, grad_w_down
```

```python
import jax
import jax.numpy as jnp
from jax import lax
from jax.sharding import Mesh
from jax.sharding import PartitionSpec as P

EXPERTS = 32
CAP = 10
TP = ("tp_0", "tp_1")
EP = ("ex", "ey")
F32 = jnp.float32
BF16 = jnp.bfloat16
ROWS = 16
LANES = 256


def swap_cores(a, chips):
    pairs = [(2 * z + c, 2 * z + 1 - c) for z in range(chips) for c in range(2)]
    return lax.ppermute(a, TP, pairs)


def summed_over_tp(part):
    chips = lax.axis_size("tp_0")
    slots, units = part.shape
    bands = chips // 2
    blocks = part.reshape(bands, slots // bands, 4, units // 4).transpose(2, 0, 1, 3)
    blocks = blocks.reshape(2, 2, bands, slots // bands, units // 4)
    core = lax.axis_index("tp_1")
    kept = lax.dynamic_index_in_dim(blocks, core, 0, False)
    given = lax.dynamic_index_in_dim(blocks, 1 - core, 0, False)
    got = swap_cores(given, chips)
    pair = (kept.astype(F32) + got.astype(F32)).astype(BF16)
    pair = pair.reshape(chips, slots // bands, units // 4)
    terms = lax.all_to_all(pair, "tp_0", 0, 0, tiled=True)
    mine = jnp.sum(terms.astype(F32), axis=0).astype(BF16)
    every = lax.all_gather(mine, TP, axis=0, tiled=False)
    every = every.reshape(2, bands, 2, slots // bands, units // 4)
    return every.transpose(1, 3, 2, 0, 4).reshape(slots, units)


def on_device(tokens, cotangent, gates, expert_ids, saved_gate, saved_up, w_gate, w_up, w_down):
    width = tokens.shape[1]
    rows = tokens.shape[0]
    experts = jnp.arange(EXPERTS, dtype=jnp.int32)
    hits = expert_ids[:, :, None] == experts[None, None, :]
    named = jnp.sum(hits.astype(F32), axis=1)
    gate_of = jnp.sum(jnp.where(hits, gates.astype(F32)[:, :, None], 0.0), axis=1)
    order = jnp.arange(rows, dtype=jnp.int32)
    earlier = (order[:, None] > order[None, :]).astype(BF16)
    place = jnp.dot(earlier, named.astype(BF16), preferred_element_type=F32)
    place = jnp.where(named > 0, place, -1.0).T
    takes = place[:, None, :] == jnp.arange(CAP, dtype=jnp.int32).astype(F32)[None, :, None]
    table = takes.astype(BF16)
    send_x = jnp.einsum("est,td->esd", table, tokens, preferred_element_type=F32).astype(BF16)
    send_dy = jnp.einsum("est,td->esd", table, cotangent, preferred_element_type=F32).astype(BF16)
    send_g = jnp.sum(jnp.where(takes, gate_of.T[:, None, :], 0.0), axis=2, keepdims=True).astype(BF16)
    send_dy = jnp.concatenate([send_dy, send_g], axis=2)
    send_dy = jnp.pad(send_dy, ((0, 0), (0, ROWS - CAP), (0, LANES - width - 1)))
    send_x = jnp.pad(send_x, ((0, 0), (0, ROWS - CAP), (0, LANES - width)))
    recv_dy = lax.all_to_all(send_dy, EP, 0, 0, tiled=True)
    recv_x = lax.all_to_all(send_x, EP, 0, 0, tiled=True)
    recv_dy = recv_dy[:, :CAP].reshape(EXPERTS * CAP, LANES)
    gate = recv_dy[:, width : width + 1].astype(F32)
    dy = recv_dy[:, :width]
    x = recv_x[:, :CAP, :width].reshape(EXPERTS * CAP, width)

    act_gate = saved_gate[:, 0, :].T.astype(F32)
    act_up = saved_up[:, 0, :].T.astype(F32)
    down = w_down[0].T
    part = jnp.dot(dy, down, preferred_element_type=F32).astype(BF16)
    total = summed_over_tp(part).astype(F32)

    scaled = (gate * dy.astype(F32)).astype(BF16)
    sigm = jax.nn.sigmoid(act_gate)
    hidden = (act_gate * sigm * act_up).astype(BF16)
    score = jnp.sum(hidden.astype(F32) * total, axis=1, keepdims=True).astype(BF16)
    dh = gate * total
    d_gate = (dh * act_up * sigm * (1.0 + act_gate * (1.0 - sigm))).astype(BF16)
    d_up = (dh * act_gate * sigm).astype(BF16)
    over_units = (((1,), (1,)), ((), ()))
    dx = lax.dot_general(d_gate, w_gate[0], over_units, preferred_element_type=F32)
    dx = dx + lax.dot_general(d_up, w_up[0], over_units, preferred_element_type=F32)
    back = jnp.concatenate([dx.astype(BF16), score], axis=1).reshape(EXPERTS, CAP, width + 1)
    back = jnp.pad(back, ((0, 0), (0, ROWS - CAP), (0, LANES - width - 1)))
    home = lax.all_to_all(back, EP, 0, 0, tiled=True)

    over_slots = (((0,), (0,)), ((), ()))
    grad_w_gate = lax.dot_general(x, d_gate, over_slots, preferred_element_type=F32).astype(BF16)
    grad_w_up = lax.dot_general(x, d_up, over_slots, preferred_element_type=F32).astype(BF16)
    grad_w_down = lax.dot_general(scaled, hidden, over_slots, preferred_element_type=F32).astype(BF16)

    home = home[:, :CAP].reshape(EXPERTS * CAP, LANES)
    flat = table.reshape(EXPERTS * CAP, rows)
    grad_tokens = lax.dot_general(flat, home[:, :width], over_slots, preferred_element_type=F32).astype(BF16)
    score_home = home[:, width].reshape(EXPERTS, CAP).astype(F32)
    of_pair = jnp.sum(jnp.where(takes, score_home[:, :, None], 0.0), axis=1)
    grad_gates = jnp.sum(jnp.where(hits, of_pair.T[:, None, :], 0.0), axis=2).astype(BF16)
    return (grad_tokens, grad_gates, grad_w_gate[None], grad_w_up[None], grad_w_down.T[None])


def solution(mesh):
    split = Mesh(
        mesh.devices.reshape(mesh.shape["ex"], mesh.shape["ey"], mesh.shape["tp"] // 2, 2),
        ("ex", "ey", "tp_0", "tp_1"),
    )
    in_specs = (
        P(EP, TP),
        P(EP, TP),
        P(EP, None),
        P(EP, None),
        P(None, EP, None),
        P(None, EP, None),
        P(EP, TP, None),
        P(EP, TP, None),
        P(EP, None, TP),
    )
    out_specs = (
        P(EP, TP),
        P(EP, None),
        P(EP, TP, None),
        P(EP, TP, None),
        P(EP, None, TP),
    )
    return jax.shard_map(
        on_device, mesh=split, in_specs=in_specs, out_specs=out_specs, check_vma=False
    )
```

```python
import jax
import jax.numpy as jnp
from jax import lax
from jax.experimental import pallas as pl
from jax.experimental.pallas import tpu as pltpu
from jax.sharding import Mesh
from jax.sharding import PartitionSpec as P

EXPERTS = 32
TOP = 8
CAP = 10
ROWS = 32
WIDTH = 224
UNITS = 1024
SLOTS = 320
PACK = 40
HOME = 16
TP = ("tp_0", "tp_1")
EP = ("ex", "ey")
F32 = jnp.float32
BF16 = jnp.bfloat16
VMEM = pl.BlockSpec(memory_space=pltpu.VMEM)
SMEM = pl.BlockSpec(memory_space=pltpu.SMEM)
OVER_UNITS = (((1,), (1,)), ((), ()))
OVER_ROWS = (((0,), (0,)), ((), ()))


def iota(shape, dim):
    return lax.broadcasted_iota(jnp.int32, shape, dim)


def dot(a, b, dims=(((1,), (0,)), ((), ()))):
    return lax.dot_general(a, b, dims, preferred_element_type=F32)


def places(ids, gates):
    expert = iota((EXPERTS, ROWS), 0)
    named = jnp.zeros((EXPERTS, ROWS), F32)
    weight = jnp.zeros((EXPERTS, ROWS), F32)
    for k in range(TOP):
        hit = ids[k : k + 1, :] == expert
        named = named + jnp.where(hit, 1.0, 0.0)
        if gates is not None:
            weight = weight + jnp.where(hit, gates[k : k + 1, :], 0.0)
    before = jnp.where(iota((ROWS, ROWS), 0) < iota((ROWS, ROWS), 1), 1.0, 0.0).astype(BF16)
    place = dot(named.astype(BF16), before)
    return jnp.where(named > 0.5, place, -1.0), weight


def pack_kernel(ids_ref, gates_ref, tok_ref, cot_ref, out_ref):
    place, weight = places(ids_ref[...], gates_ref[...].astype(F32))
    place = jnp.concatenate([place] * 4, axis=1)
    weight = jnp.concatenate([weight] * 4, axis=1)
    row, lane = iota((PACK, 128), 0), iota((PACK, 128), 1)
    want = row - CAP * (lane // ROWS)
    want = jnp.where((want >= 0) & (want < CAP), want, -2).astype(F32)
    tail = lane >= 3 * ROWS
    tok, cot = tok_ref[...], cot_ref[...]
    zeros = jnp.zeros((ROWS, 64), BF16)
    source = jnp.concatenate(
        [
            tok[:, :128],
            cot[:, :128],
            jnp.concatenate([tok[:, 128:192], cot[:, 128:192]], axis=1),
            jnp.concatenate([tok[:, 192:224], cot[:, 192:224], zeros], axis=1),
        ],
        axis=0,
    )
    at_gate = jnp.where(iota((128, 128), 1) == 64, 1.0, 0.0).astype(BF16)
    for e in range(EXPERTS):
        takes = place[e : e + 1, :] == want
        pick = jnp.where(takes, 1.0, 0.0).astype(BF16)
        gate = jnp.where(takes & tail, weight[e : e + 1, :], 0.0).astype(BF16)
        out_ref[e] = (dot(pick, source) + dot(gate, at_gate)).astype(BF16)


def product_kernel(core_ref, recv_ref, down_ref, kept_ref, given_ref, x_ref, scaled_ref, gate_ref):
    core = core_ref[0]
    to_x = jnp.concatenate([iota((128, 128), 1), iota((128, 128), 1)], axis=0)
    at = iota((256, 128), 0)
    from_x = jnp.where(to_x < 64, to_x, to_x + 64)
    from_x = jnp.where(to_x < 96, from_x, -1)
    from_dy = jnp.where(to_x < 64, to_x + 64, to_x + 96)
    from_dy = jnp.where(to_x < 96, from_dy, -1)
    x_move = jnp.where(at == from_x, 1.0, 0.0).astype(BF16)
    dy_move = jnp.where(at == from_dy, 1.0, 0.0).astype(BF16)
    slot, place = iota((8 * CAP, 8 * PACK), 0), iota((8 * CAP, 8 * PACK), 1)
    base = (slot // CAP) * PACK + slot % CAP
    picks = [jnp.where(place == base + CAP * kind, 1.0, 0.0).astype(BF16) for kind in range(4)]
    dys = []
    for j in range(4):
        got = recv_ref[8 * j : 8 * j + 8].reshape(8 * PACK, 128)
        x_low, dy_low, middle, last = [dot(pick, got) for pick in picks]
        tail = jnp.concatenate([middle, last], axis=1).astype(BF16)
        x_high = dot(tail, x_move)
        dy_high = dot(tail, dy_move)
        x = jnp.concatenate([x_low, x_high[:, :96]], axis=1)
        dy = jnp.concatenate([dy_low, dy_high[:, :96]], axis=1)
        gate = last[:, 64:65]
        rows = slice(8 * CAP * j, 8 * CAP * (j + 1))
        x_ref[rows, :] = x.astype(BF16)
        scaled_ref[rows, :] = (gate * dy).astype(BF16)
        gate_ref[rows, :] = jnp.broadcast_to(gate, (8 * CAP, 128))
        dys.append(dy.astype(BF16))
    dy = jnp.concatenate(dys, axis=0)
    low, high = down_ref[:, :512], down_ref[:, 512:]
    for ref, first in ((given_ref, core == 1), (kept_ref, core == 0)):
        part = dot(dy, jnp.where(first, low, high))
        for v in range(2):
            for b in range(8):
                ref[8 * v + b] = part[40 * b : 40 * b + 40, 256 * v : 256 * v + 256].astype(BF16)


def factors_kernel(gate_ref, up_ref, hidden_ref, by_gate_ref, by_up_ref):
    for b in range(20):
        rows = slice(16 * b, 16 * b + 16)
        gate = gate_ref[rows, :].astype(F32)
        up = up_ref[rows, :].astype(F32)
        sigm = jax.nn.sigmoid(gate)
        by_up = gate * sigm
        hidden_ref[rows, :] = (by_up * up).astype(BF16)
        by_gate_ref[rows, :] = up * sigm * (1.0 + gate * (1.0 - sigm))
        by_up_ref[rows, :] = by_up


def down_kernel(scaled_ref, hidden_ref, wd_ref):
    wd_ref[...] = dot(scaled_ref[...], hidden_ref[...], OVER_ROWS).astype(BF16)


def weights_kernel(x_ref, dg_ref, du_ref, wg_ref, wu_ref):
    wg_ref[...] = dot(x_ref[...], dg_ref[...], OVER_ROWS).astype(BF16)
    wu_ref[...] = dot(x_ref[...], du_ref[...], OVER_ROWS).astype(BF16)


def pair_kernel(kept_ref, got_ref, pair_ref):
    for z in range(kept_ref.shape[0]):
        pair_ref[z] = (kept_ref[z].astype(F32) + got_ref[z].astype(F32)).astype(BF16)


def spread_kernel(terms_ref, copies_ref):
    total = terms_ref[0].astype(F32)
    for z in range(1, terms_ref.shape[0]):
        total = total + terms_ref[z].astype(F32)
    total = total.astype(BF16)
    for z in range(terms_ref.shape[0]):
        copies_ref[z] = total


def grads_kernel(core_ref, own_ref, other_ref, gate_ref, by_gate_ref, by_up_ref, hidden_ref, wg_ref, wu_ref, dg_ref, du_ref, back_ref, dx_ref):
    core = core_ref[0]
    for b in range(8):
        rows = slice(40 * b, 40 * b + 40)
        gate = gate_ref[rows, 0:1]
        score = jnp.zeros((40, 1), F32)
        for c in range(2):
            for v in range(2):
                units = slice(512 * c + 256 * v, 512 * c + 256 * v + 256)
                total = jnp.where(core == c, own_ref[8 * v + b], other_ref[8 * v + b]).astype(F32)
                dh = gate * total
                dg_ref[rows, units] = (dh * by_gate_ref[rows, units]).astype(BF16)
                du_ref[rows, units] = (dh * by_up_ref[rows, units]).astype(BF16)
                score = score + jnp.sum(total * hidden_ref[rows, units].astype(F32), axis=1, keepdims=True)
        dx_ref[rows, :] = jnp.broadcast_to(score, (40, 256))
    dx = dot(dg_ref[...], wg_ref[...], OVER_UNITS) + dot(du_ref[...], wu_ref[...], OVER_UNITS)
    dx_ref[:, :WIDTH] = dx
    out, row = iota((8 * HOME, 8 * CAP), 0), iota((8 * HOME, 8 * CAP), 1)
    spread = (row // CAP == out // HOME) & (row % CAP == out % HOME)
    spread = jnp.where(spread, 1.0, 0.0).astype(BF16)
    for j in range(4):
        block = dx_ref[8 * CAP * j : 8 * CAP * (j + 1), :].astype(BF16)
        back_ref[8 * j : 8 * j + 8] = dot(spread, block).astype(BF16).reshape(8, HOME, 256)


def home_kernel(ids_ref, home_ref, tok_ref, gates_ref):
    ids = ids_ref[...]
    place, _ = places(ids, None)
    slot = iota((HOME, ROWS), 0).astype(F32)
    table = jnp.concatenate([jnp.where(place[e : e + 1, :] == slot, 1.0, 0.0) for e in range(EXPERTS)], axis=0)
    home = home_ref[...].reshape(EXPERTS * HOME, 256)
    tok_ref[...] = dot(table.astype(BF16), home, OVER_ROWS)[:, :WIDTH].astype(BF16)
    score = home[:, WIDTH : WIDTH + 1].astype(F32)
    of_pair = jnp.sum((table * score).reshape(EXPERTS, HOME, ROWS), axis=1)
    expert = iota((EXPERTS, ROWS), 0)
    for k in range(TOP):
        hit = ids[k : k + 1, :] == expert
        gates_ref[k : k + 1, :] = jnp.sum(jnp.where(hit, of_pair, 0.0), axis=0, keepdims=True).astype(BF16)


def near(array):
    return pltpu.with_memory_space_constraint(array, pltpu.VMEM)


def call(body, outs, args, scratch=(), name=None, room=16):
    specs = [SMEM if a.dtype == jnp.int32 and a.ndim == 1 else VMEM for a in args]
    return pl.pallas_call(
        body,
        out_shape=[
            pltpu.VMEM(shape, dtype) if stays else jax.ShapeDtypeStruct(shape, dtype)
            for shape, dtype, stays in outs
        ],
        in_specs=specs,
        out_specs=[VMEM] * len(outs),
        scratch_shapes=list(scratch),
        compiler_params=pltpu.CompilerParams(vmem_limit_bytes=room * 1024 * 1024),
        name=name,
    )(*args)


def on_device(tokens, cotangent, gates, expert_ids, saved_gate, saved_up, w_gate, w_up, w_down):
    ids = expert_ids.T
    core = lax.axis_index("tp_1").reshape(1)
    chips = lax.axis_size("tp_0")
    pairs = [(2 * z + c, 2 * z + 1 - c) for z in range(chips) for c in range(2)]
    send = call(
        pack_kernel, [((EXPERTS, PACK, 128), BF16, False)], [ids, gates.T, tokens, cotangent], name="pack", room=60
    )[0]
    recv = lax.all_to_all(send, EP, 0, 0, tiled=True)
    units = ((SLOTS, UNITS), BF16, True)
    wide = ((SLOTS, UNITS), F32, True)
    hidden, by_gate, by_up = call(
        factors_kernel,
        [units, wide, wide],
        [near(saved_gate[:, 0, :].T), near(saved_up[:, 0, :].T)],
        name="factors",
    )
    recv, hidden, by_gate, by_up = lax.optimization_barrier((recv, hidden, by_gate, by_up))
    half = ((chips, 40, 256), BF16, True)
    kept, given, x, scaled, gate = call(
        product_kernel,
        [half, half, ((SLOTS, WIDTH), BF16, False), ((SLOTS, WIDTH), BF16, True), ((SLOTS, 128), F32, True)],
        [core, near(recv), near(w_down[0].T)],
        name="product",
    )
    weights = ((WIDTH, UNITS), BF16, False)
    got = lax.ppermute(given, TP, pairs)
    grad_w_down = call(down_kernel, [weights], [near(scaled), near(hidden)], name="down")[0]
    got, grad_w_down = lax.optimization_barrier((got, grad_w_down))
    pair = call(pair_kernel, [half], [near(kept), near(got)], name="pair")[0]
    terms = lax.all_to_all(pair, "tp_0", 0, 0, tiled=True)

    copies = call(spread_kernel, [((chips, 40, 256), BF16, False)], [near(terms)], name="spread")[0]
    own = lax.all_to_all(copies, "tp_0", 0, 0, tiled=True)
    other = lax.ppermute(own, TP, pairs)
    d_gate, d_up, back = call(
        grads_kernel,
        [units, units, ((EXPERTS, HOME, 256), BF16, False)],
        [core, near(own), near(other), near(gate), near(by_gate), near(by_up), near(hidden), near(w_gate[0]), near(w_up[0])],
        scratch=[pltpu.VMEM((SLOTS, 256), F32)],
        name="grads",
    )
    home = lax.all_to_all(back, EP, 0, 0, tiled=True)
    grad_w_gate, grad_w_up = call(
        weights_kernel, [weights, weights], [near(x), near(d_gate), near(d_up)], name="weights"
    )
    grad_tokens, grad_gates = call(
        home_kernel, [((ROWS, WIDTH), BF16, False), ((TOP, ROWS), BF16, False)], [ids, near(home)], name="home"
    )
    return (grad_tokens, grad_gates.T, grad_w_gate[None], grad_w_up[None], grad_w_down.T[None])


def solution(mesh):
    split = Mesh(
        mesh.devices.reshape(mesh.shape["ex"], mesh.shape["ey"], mesh.shape["tp"] // 2, 2),
        ("ex", "ey", "tp_0", "tp_1"),
    )
    in_specs = (
        P(EP, TP),
        P(EP, TP),
        P(EP, None),
        P(EP, None),
        P(None, EP, None),
        P(None, EP, None),
        P(EP, TP, None),
        P(EP, TP, None),
        P(EP, None, TP),
    )
    out_specs = (
        P(EP, TP),
        P(EP, None),
        P(EP, TP, None),
        P(EP, TP, None),
        P(EP, None, TP),
    )
    return jax.shard_map(
        on_device, mesh=split, in_specs=in_specs, out_specs=out_specs, check_vma=False
    )
```

```python
import jax
import jax.numpy as jnp
from jax import lax
from jax.experimental import pallas as pl
from jax.experimental.pallas import tpu as pltpu
from jax.sharding import Mesh
from jax.sharding import PartitionSpec as P

EXPERTS = 32
TOP = 8
CAP = 10
ROWS = 32
WIDTH = 224
UNITS = 1024
SLOTS = 320
PACK = 40
HOME = 24
STAGGER = 9000
TP = ("tp_0", "tp_1")
EP = ("ex", "ey")
F32 = jnp.float32
BF16 = jnp.bfloat16
VMEM = pl.BlockSpec(memory_space=pltpu.VMEM)
SMEM = pl.BlockSpec(memory_space=pltpu.SMEM)
ANY = pl.BlockSpec(memory_space=pl.ANY)
OVER_UNITS = (((1,), (1,)), ((), ()))
OVER_ROWS = (((0,), (0,)), ((), ()))


def iota(shape, dim):
    return lax.broadcasted_iota(jnp.int32, shape, dim)


def dot(a, b, dims=(((1,), (0,)), ((), ()))):
    return lax.dot_general(a, b, dims, preferred_element_type=F32)


def places(ids, gates):
    expert = iota((EXPERTS, ROWS), 0)
    named = jnp.zeros((EXPERTS, ROWS), F32)
    weight = jnp.zeros((EXPERTS, ROWS), F32)
    for k in range(TOP):
        hit = ids[k : k + 1, :] == expert
        named = named + jnp.where(hit, 1.0, 0.0)
        if gates is not None:
            weight = weight + jnp.where(hit, gates[k : k + 1, :], 0.0)
    before = jnp.where(iota((ROWS, ROWS), 0) < iota((ROWS, ROWS), 1), 1.0, 0.0).astype(BF16)
    place = dot(named.astype(BF16), before)
    return jnp.where(named > 0.5, place, -1.0), weight


def pack_kernel(ids_ref, gates_ref, tok_ref, cot_ref, out_ref):
    place, weight = places(ids_ref[...], gates_ref[...].astype(F32))
    place = jnp.concatenate([place] * 4, axis=1)
    weight = jnp.concatenate([weight] * 4, axis=1)
    row, lane = iota((PACK, 128), 0), iota((PACK, 128), 1)
    want = row - CAP * (lane // ROWS)
    want = jnp.where((want >= 0) & (want < CAP), want, -2).astype(F32)
    tail = lane >= 3 * ROWS
    tok, cot = tok_ref[...], cot_ref[...]
    zeros = jnp.zeros((ROWS, 64), BF16)
    source = jnp.concatenate(
        [
            tok[:, :128],
            cot[:, :128],
            jnp.concatenate([tok[:, 128:192], cot[:, 128:192]], axis=1),
            jnp.concatenate([tok[:, 192:224], cot[:, 192:224], zeros], axis=1),
        ],
        axis=0,
    )
    at_gate = jnp.where(iota((128, 128), 1) == 64, 1.0, 0.0).astype(BF16)
    source = jnp.concatenate([source, at_gate], axis=0)
    picks = []
    for e in range(EXPERTS):
        takes = place[e : e + 1, :] == want
        pick = jnp.where(takes, 1.0, 0.0)
        gate = jnp.where(takes & tail, weight[e : e + 1, :], 0.0)
        picks.append(jnp.concatenate([pick, gate], axis=1))
    for j in range(4):
        part = jnp.concatenate(picks[8 * j : 8 * j + 8], axis=0).astype(BF16)
        out_ref[8 * j : 8 * j + 8] = dot(part, source).astype(BF16).reshape(8, PACK, 128)


def product_kernel(core_ref, recv_ref, down_ref, kept_ref, given_ref, x_ref, scaled_ref, gate_ref):
    core = core_ref[0]
    to_x = jnp.concatenate([iota((128, 128), 1), iota((128, 128), 1)], axis=0)
    at = iota((256, 128), 0)
    from_x = jnp.where(to_x < 64, to_x, to_x + 64)
    from_x = jnp.where(to_x < 96, from_x, -1)
    from_dy = jnp.where(to_x < 64, to_x + 64, to_x + 96)
    from_dy = jnp.where(to_x < 96, from_dy, -1)
    x_move = jnp.where(at == from_x, 1.0, 0.0).astype(BF16)
    dy_move = jnp.where(at == from_dy, 1.0, 0.0).astype(BF16)
    slot, place = iota((8 * CAP, 8 * PACK), 0), iota((8 * CAP, 8 * PACK), 1)
    base = (slot // CAP) * PACK + slot % CAP
    picks = [jnp.where(place == base + CAP * kind, 1.0, 0.0).astype(BF16) for kind in range(4)]
    dys = []
    for j in range(4):
        got = recv_ref[8 * j : 8 * j + 8].reshape(8 * PACK, 128)
        x_low, dy_low, middle, last = [dot(pick, got) for pick in picks]
        tail = jnp.concatenate([middle, last], axis=1).astype(BF16)
        x_high = dot(tail, x_move)
        dy_high = dot(tail, dy_move)
        x = jnp.concatenate([x_low, x_high[:, :96]], axis=1)
        dy = jnp.concatenate([dy_low, dy_high[:, :96]], axis=1)
        gate = last[:, 64:65]
        rows = slice(8 * CAP * j, 8 * CAP * (j + 1))
        x_ref[rows, :] = x.astype(BF16)
        scaled_ref[rows, :] = (gate * dy).astype(BF16)
        gate_ref[rows, :] = jnp.broadcast_to(gate, (8 * CAP, 128))
        dys.append(dy.astype(BF16))
    dy = jnp.concatenate(dys, axis=0)
    low, high = down_ref[:, :512], down_ref[:, 512:]
    for ref, first in ((given_ref, core == 1), (kept_ref, core == 0)):
        part = dot(dy, jnp.where(first, low, high))
        for v in range(2):
            for b in range(8):
                ref[8 * v + b] = part[40 * b : 40 * b + 40, 256 * v : 256 * v + 256].astype(BF16)


def factors_kernel(gate_ref, up_ref, hidden_ref, by_gate_ref, by_up_ref):
    for b in range(20):
        rows = slice(16 * b, 16 * b + 16)
        gate = gate_ref[rows, :].astype(F32)
        up = up_ref[rows, :].astype(F32)
        sigm = jax.nn.sigmoid(gate)
        by_up = gate * sigm
        hidden_ref[rows, :] = (by_up * up).astype(BF16)
        by_gate_ref[rows, :] = (up * sigm * (1.0 + gate * (1.0 - sigm))).astype(BF16)
        by_up_ref[rows, :] = by_up.astype(BF16)


def down_kernel(scaled_ref, hidden_ref, wd_ref):
    wd_ref[...] = dot(scaled_ref[...], hidden_ref[...], OVER_ROWS).astype(BF16)


def weights_kernel(core_ref, x_ref, own_dg_ref, own_du_ref, dg_ref, du_ref, wg_ref, wu_ref):
    core = core_ref[0]
    for half, dg, du in ((core, own_dg_ref, own_du_ref), (1 - core, dg_ref, du_ref)):
        units = pl.ds(pl.multiple_of(512 * half, 512), 512)
        wg_ref[:, units] = dot(x_ref[...], dg[...], OVER_ROWS).astype(BF16)
        wu_ref[:, units] = dot(x_ref[...], du[...], OVER_ROWS).astype(BF16)


def pair_kernel(core_ref, kept_ref, got_ref, pair_ref):
    @pl.when(core_ref[0] == 1)
    def _():
        pl.delay(STAGGER)

    for z in range(kept_ref.shape[0]):
        pair_ref[z] = (kept_ref[z].astype(F32) + got_ref[z].astype(F32)).astype(BF16)


def spread_kernel(terms_ref, copies_ref):
    total = terms_ref[0].astype(F32)
    for z in range(1, terms_ref.shape[0]):
        total = total + terms_ref[z].astype(F32)
    total = total.astype(BF16)
    for z in range(terms_ref.shape[0]):
        copies_ref[z] = total


def half_grads(half, half_ref, gate_ref, by_gate_ref, by_up_ref, hidden_ref, wg_ref, wu_ref, dg_out, du_out, dx_ref, dg_ref, du_ref, done, first):
    for b in range(8):
        rows = slice(40 * b, 40 * b + 40)
        gate = gate_ref[rows, 0:1]
        score = jnp.zeros((40, 1), F32)
        for v in range(2):
            units = pl.ds(pl.multiple_of(512 * half + 256 * v, 256), 256)
            here = slice(256 * v, 256 * v + 256)
            total = half_ref[8 * v + b].astype(F32)
            dh = gate * total
            dg_ref[rows, here] = (dh * by_gate_ref[rows, units].astype(F32)).astype(BF16)
            du_ref[rows, here] = (dh * by_up_ref[rows, units].astype(F32)).astype(BF16)
            score = score + jnp.sum(total * hidden_ref[rows, units].astype(F32), axis=1, keepdims=True)
        score = jnp.broadcast_to(score, (40, 256 - WIDTH))
        dx_ref[rows, WIDTH:] = score if first else dx_ref[rows, WIDTH:] + score
    copies = [pltpu.make_async_copy(dg_ref, dg_out, done.at[0]), pltpu.make_async_copy(du_ref, du_out, done.at[1])]
    for copy in copies:
        copy.start()
    units = pl.ds(pl.multiple_of(512 * half, 512), 512)
    dx = dot(dg_ref[...], wg_ref[:, units], OVER_UNITS) + dot(du_ref[...], wu_ref[:, units], OVER_UNITS)
    dx_ref[:, :WIDTH] = dx if first else dx_ref[:, :WIDTH] + dx
    return copies


def own_kernel(core_ref, *refs):
    for copy in half_grads(core_ref[0], *refs, True):
        copy.wait()


def other_kernel(core_ref, *refs):
    shared, own_ref, dg_out, du_out, back_ref, dx_ref, scratch = refs[:7], *refs[7:12], refs[12:]
    dx_ref[...] = own_ref[...]
    copies = half_grads(1 - core_ref[0], *shared, dg_out, du_out, dx_ref, *scratch, False)
    out, row = iota((8 * HOME, 8 * CAP), 0), iota((8 * HOME, 8 * CAP), 1)
    block, place = out // HOME, out % HOME
    same = row // CAP == block
    low = jnp.where(same & (row % CAP == place), 1.0, 0.0).astype(BF16)
    high = jnp.where(same & (row % CAP == place - CAP), 1.0, 0.0).astype(BF16)
    for j in range(4):
        rows = slice(8 * CAP * j, 8 * CAP * (j + 1))
        spread = dot(low, dx_ref[rows, :128].astype(BF16)) + dot(high, dx_ref[rows, 128:].astype(BF16))
        back_ref[8 * j : 8 * j + 8] = spread.astype(BF16).reshape(8, HOME, 128)
    for copy in copies:
        copy.wait()


def home_kernel(ids_ref, home_ref, tok_ref, gates_ref):
    ids = ids_ref[...]
    place, _ = places(ids, None)
    slot = iota((HOME, ROWS), 0).astype(F32)
    tables = [jnp.where(place[e : e + 1, :] == slot, 1.0, 0.0) for e in range(EXPERTS)]
    table = jnp.concatenate(tables, axis=0)
    past = jnp.where(place >= 0.0, place + CAP, -1.0)
    later = jnp.concatenate([jnp.where(past[e : e + 1, :] == slot, 1.0, 0.0) for e in range(EXPERTS)], axis=0)
    home = home_ref[...].reshape(EXPERTS * HOME, 128)
    tok_ref[:, :128] = dot(table.astype(BF16), home, OVER_ROWS).astype(BF16)
    tok_ref[:, 128:] = dot(later.astype(BF16), home, OVER_ROWS)[:, : WIDTH - 128].astype(BF16)
    score = home[:, WIDTH - 128 : WIDTH - 127].astype(F32)
    of_pair = jnp.sum((later * score).reshape(EXPERTS, HOME, ROWS), axis=1)
    expert = iota((EXPERTS, ROWS), 0)
    for k in range(TOP):
        hit = ids[k : k + 1, :] == expert
        gates_ref[k : k + 1, :] = jnp.sum(jnp.where(hit, of_pair, 0.0), axis=0, keepdims=True).astype(BF16)


def near(array):
    return pltpu.with_memory_space_constraint(array, pltpu.VMEM)


def call(body, outs, args, scratch=(), name=None, room=16):
    specs = [SMEM if a.dtype == jnp.int32 and a.ndim == 1 else VMEM for a in args]
    return pl.pallas_call(
        body,
        out_shape=[
            pltpu.VMEM(shape, dtype) if stays else jax.ShapeDtypeStruct(shape, dtype)
            for shape, dtype, stays in outs
        ],
        in_specs=specs,
        out_specs=[ANY if stays is None else VMEM for _, _, stays in outs],
        scratch_shapes=list(scratch),
        compiler_params=pltpu.CompilerParams(vmem_limit_bytes=room * 1024 * 1024),
        name=name,
    )(*args)


def on_device(tokens, cotangent, gates, expert_ids, saved_gate, saved_up, w_gate, w_up, w_down):
    ids = expert_ids.T
    core = lax.axis_index("tp_1").reshape(1)
    chips = lax.axis_size("tp_0")
    pairs = [(2 * z + c, 2 * z + 1 - c) for z in range(chips) for c in range(2)]
    send = call(
        pack_kernel, [((EXPERTS, PACK, 128), BF16, False)], [ids, gates.T, tokens, cotangent], name="pack", room=60
    )[0]
    recv = lax.all_to_all(send, EP, 0, 0, tiled=True)
    units = ((SLOTS, UNITS), BF16, True)
    hidden, by_gate, by_up = call(
        factors_kernel,
        [units, units, units],
        [near(saved_gate[:, 0, :].T), near(saved_up[:, 0, :].T)],
        name="factors",
    )
    recv, hidden, by_gate, by_up = lax.optimization_barrier((recv, hidden, by_gate, by_up))
    half = ((chips, 40, 256), BF16, True)
    kept, given, x, scaled, gate = call(
        product_kernel,
        [half, half, ((SLOTS, WIDTH), BF16, False), ((SLOTS, WIDTH), BF16, True), ((SLOTS, 128), F32, True)],
        [core, near(recv), near(w_down[0].T)],
        name="product",
    )
    weights = ((WIDTH, UNITS), BF16, False)
    got = lax.ppermute(given, TP, pairs)
    grad_w_down = call(down_kernel, [weights], [near(scaled), near(hidden)], name="down")[0]
    got, grad_w_down = lax.optimization_barrier((got, grad_w_down))
    pair = call(pair_kernel, [half], [core, near(kept), near(got)], name="pair")[0]
    terms = lax.all_to_all(pair, "tp_0", 0, 0, tiled=True)

    copies = call(spread_kernel, [((chips, 40, 256), BF16, False)], [near(terms)], name="spread")[0]
    own = lax.all_to_all(copies, "tp_0", 0, 0, tiled=True)
    other = lax.ppermute(own, TP, pairs)
    wide_half = ((SLOTS, UNITS // 2), BF16, None)
    drafts = [pltpu.VMEM((SLOTS, UNITS // 2), BF16), pltpu.VMEM((SLOTS, UNITS // 2), BF16), pltpu.SemaphoreType.DMA((2,))]
    sums = ((SLOTS, 256), F32, True)
    shared = [near(gate), near(by_gate), near(by_up), near(hidden), near(w_gate[0]), near(w_up[0])]
    own_dg, own_du, own_dx = call(own_kernel, [wide_half, wide_half, sums], [core, near(own), *shared], drafts, name="own")
    other, own_dx = lax.optimization_barrier((other, own_dx))
    dg, du, back = call(
        other_kernel,
        [wide_half, wide_half, ((EXPERTS, HOME, 128), BF16, False)],
        [core, near(other), *shared, near(own_dx)],
        scratch=[pltpu.VMEM((SLOTS, 256), F32), *drafts],
        name="other",
    )
    home = lax.all_to_all(back, EP, 0, 0, tiled=True)
    grad_w_gate, grad_w_up = call(
        weights_kernel,
        [weights, weights],
        [core, near(x), near(own_dg), near(own_du), near(dg), near(du)],
        name="weights",
    )
    grad_tokens, grad_gates = call(
        home_kernel, [((ROWS, WIDTH), BF16, False), ((TOP, ROWS), BF16, False)], [ids, near(home)], name="home"
    )
    return (grad_tokens, grad_gates.T, grad_w_gate[None], grad_w_up[None], grad_w_down.T[None])


def solution(mesh):
    split = Mesh(
        mesh.devices.reshape(mesh.shape["ex"], mesh.shape["ey"], mesh.shape["tp"] // 2, 2),
        ("ex", "ey", "tp_0", "tp_1"),
    )
    in_specs = (
        P(EP, TP),
        P(EP, TP),
        P(EP, None),
        P(EP, None),
        P(None, EP, None),
        P(None, EP, None),
        P(EP, TP, None),
        P(EP, TP, None),
        P(EP, None, TP),
    )
    out_specs = (
        P(EP, TP),
        P(EP, None),
        P(EP, TP, None),
        P(EP, TP, None),
        P(EP, None, TP),
    )
    return jax.shard_map(
        on_device, mesh=split, in_specs=in_specs, out_specs=out_specs, check_vma=False
    )
```

```python
import jax
import jax.numpy as jnp
from jax import lax
from jax.experimental import pallas as pl
from jax.experimental.pallas import tpu as pltpu
from jax.sharding import Mesh
from jax.sharding import PartitionSpec as P

EXPERTS = 32
TOP = 8
CAP = 10
ROWS = 32
WIDTH = 224
UNITS = 1024
SLOTS = 320
PACK = 40
HOME = 24
STAGGER = 8000
TP = ("tp_0", "tp_1")
EP = ("ex", "ey")
F32 = jnp.float32
BF16 = jnp.bfloat16
VMEM = pl.BlockSpec(memory_space=pltpu.VMEM)
SMEM = pl.BlockSpec(memory_space=pltpu.SMEM)
ANY = pl.BlockSpec(memory_space=pl.ANY)
OVER_UNITS = (((1,), (1,)), ((), ()))
OVER_ROWS = (((0,), (0,)), ((), ()))


def iota(shape, dim):
    return lax.broadcasted_iota(jnp.int32, shape, dim)


def dot(a, b, dims=(((1,), (0,)), ((), ()))):
    return lax.dot_general(a, b, dims, preferred_element_type=F32)


def places(ids, gates):
    expert = iota((EXPERTS, ROWS), 0)
    named = jnp.zeros((EXPERTS, ROWS), F32)
    weight = jnp.zeros((EXPERTS, ROWS), F32)
    for k in range(TOP):
        hit = ids[k : k + 1, :] == expert
        named = named + jnp.where(hit, 1.0, 0.0)
        if gates is not None:
            weight = weight + jnp.where(hit, gates[k : k + 1, :], 0.0)
    before = jnp.where(iota((ROWS, ROWS), 0) < iota((ROWS, ROWS), 1), 1.0, 0.0).astype(BF16)
    place = dot(named.astype(BF16), before)
    return jnp.where(named > 0.5, place, -1.0), weight


def quarter(block_ref, out_ref, done, j):
    rows = pl.ds(8 * j, 8)
    return pltpu.make_async_copy(block_ref.at[rows], out_ref.at[rows], done.at[j])


def pack_kernel(ids_ref, gates_ref, tok_ref, cot_ref, out_ref, block_ref, done):
    place, weight = places(ids_ref[...], gates_ref[...].astype(F32))
    place = jnp.concatenate([place] * 4, axis=1)
    weight = jnp.concatenate([weight] * 4, axis=1)
    row, lane = iota((PACK, 128), 0), iota((PACK, 128), 1)
    want = row - CAP * (lane // ROWS)
    want = jnp.where((want >= 0) & (want < CAP), want, -2).astype(F32)
    tail = lane >= 3 * ROWS
    tok, cot = tok_ref[...], cot_ref[...]
    zeros = jnp.zeros((ROWS, 64), BF16)
    source = jnp.concatenate(
        [
            tok[:, :128],
            cot[:, :128],
            jnp.concatenate([tok[:, 128:192], cot[:, 128:192]], axis=1),
            jnp.concatenate([tok[:, 192:224], cot[:, 192:224], zeros], axis=1),
        ],
        axis=0,
    )
    at_gate = jnp.where(iota((128, 128), 1) == 64, 1.0, 0.0).astype(BF16)
    source = jnp.concatenate([source, at_gate], axis=0)
    picks = []
    for e in range(EXPERTS):
        takes = place[e : e + 1, :] == want
        pick = jnp.where(takes, 1.0, 0.0)
        gate = jnp.where(takes & tail, weight[e : e + 1, :], 0.0)
        picks.append(jnp.concatenate([pick, gate], axis=1))
    for j in range(4):
        part = jnp.concatenate(picks[8 * j : 8 * j + 8], axis=0).astype(BF16)
        block_ref[8 * j : 8 * j + 8] = dot(part, source).astype(BF16).reshape(8, PACK, 128)
        quarter(block_ref, out_ref, done, j).start()
    for j in range(4):
        quarter(block_ref, out_ref, done, j).wait()


def half_product(dy, first, down_ref, out_ref):
    part = dot(dy, jnp.where(first, down_ref[:, :512], down_ref[:, 512:]))
    for v in range(2):
        for b in range(8):
            out_ref[8 * v + b] = part[40 * b : 40 * b + 40, 256 * v : 256 * v + 256].astype(BF16)


def kept_kernel(core_ref, dy_ref, down_ref, scaled_ref, hidden_ref, kept_ref, wd_ref):
    half_product(dy_ref[...], core_ref[0] == 0, down_ref, kept_ref)
    wd_ref[...] = dot(scaled_ref[...], hidden_ref[...], OVER_ROWS).astype(BF16)


def product_kernel(core_ref, recv_ref, down_ref, given_ref, dy_ref, x_ref, scaled_ref, gate_ref):
    to_x = jnp.concatenate([iota((128, 128), 1), iota((128, 128), 1)], axis=0)
    at = iota((256, 128), 0)
    from_x = jnp.where(to_x < 64, to_x, to_x + 64)
    from_x = jnp.where(to_x < 96, from_x, -1)
    from_dy = jnp.where(to_x < 64, to_x + 64, to_x + 96)
    from_dy = jnp.where(to_x < 96, from_dy, -1)
    x_move = jnp.where(at == from_x, 1.0, 0.0).astype(BF16)
    dy_move = jnp.where(at == from_dy, 1.0, 0.0).astype(BF16)
    slot, place = iota((8 * CAP, 8 * PACK), 0), iota((8 * CAP, 8 * PACK), 1)
    base = (slot // CAP) * PACK + slot % CAP
    picks = [jnp.where(place == base + CAP * kind, 1.0, 0.0).astype(BF16) for kind in range(4)]
    for j in range(4):
        got = recv_ref[8 * j : 8 * j + 8].reshape(8 * PACK, 128)
        x_low, dy_low, middle, last = [dot(pick, got) for pick in picks]
        tail = jnp.concatenate([middle, last], axis=1).astype(BF16)
        x_high = dot(tail, x_move)
        dy_high = dot(tail, dy_move)
        x = jnp.concatenate([x_low, x_high[:, :96]], axis=1)
        dy = jnp.concatenate([dy_low, dy_high[:, :96]], axis=1)
        gate = last[:, 64:65]
        rows = slice(8 * CAP * j, 8 * CAP * (j + 1))
        x_ref[rows, :] = x.astype(BF16)
        scaled_ref[rows, :] = (gate * dy).astype(BF16)
        gate_ref[rows, :] = jnp.broadcast_to(gate, (8 * CAP, 128))
        dy_ref[rows, :] = dy.astype(BF16)
    half_product(dy_ref[...], core_ref[0] == 1, down_ref, given_ref)


def factors_kernel(gate_ref, up_ref, hidden_ref, by_gate_ref, by_up_ref):
    for b in range(20):
        rows = slice(16 * b, 16 * b + 16)
        gate = gate_ref[rows, :].astype(F32)
        up = up_ref[rows, :].astype(F32)
        sigm = jax.nn.sigmoid(gate)
        by_up = gate * sigm
        hidden_ref[rows, :] = (by_up * up).astype(BF16)
        by_gate_ref[rows, :] = (up * sigm * (1.0 + gate * (1.0 - sigm))).astype(BF16)
        by_up_ref[rows, :] = by_up.astype(BF16)


def weights_kernel(core_ref, x_ref, own_dg_ref, own_du_ref, dg_ref, du_ref, wg_ref, wu_ref):
    core = core_ref[0]
    for half, dg, du in ((core, own_dg_ref, own_du_ref), (1 - core, dg_ref, du_ref)):
        units = pl.ds(pl.multiple_of(512 * half, 512), 512)
        wg_ref[:, units] = dot(x_ref[...], dg[...], OVER_ROWS).astype(BF16)
        wu_ref[:, units] = dot(x_ref[...], du[...], OVER_ROWS).astype(BF16)


def pair_kernel(core_ref, kept_ref, got_ref, pair_ref):
    @pl.when(core_ref[0] == 1)
    def _():
        pl.delay(STAGGER)

    for z in range(kept_ref.shape[0]):
        pair_ref[z] = (kept_ref[z].astype(F32) + got_ref[z].astype(F32)).astype(BF16)


def spread_kernel(terms_ref, copies_ref):
    total = terms_ref[0].astype(F32)
    for z in range(1, terms_ref.shape[0]):
        total = total + terms_ref[z].astype(F32)
    total = total.astype(BF16)
    for z in range(terms_ref.shape[0]):
        copies_ref[z] = total


def half_grads(half, half_ref, gate_ref, by_gate_ref, by_up_ref, hidden_ref, wg_ref, wu_ref, before_ref, dg_out, du_out, dx_ref, dg_ref, du_ref, done):
    for b in range(8):
        rows = slice(40 * b, 40 * b + 40)
        gate = gate_ref[rows, 0:1]
        score = jnp.zeros((40, 1), F32)
        for v in range(2):
            units = pl.ds(pl.multiple_of(512 * half + 256 * v, 256), 256)
            here = slice(256 * v, 256 * v + 256)
            total = half_ref[8 * v + b].astype(F32)
            dh = gate * total
            dg_ref[rows, here] = (dh * by_gate_ref[rows, units].astype(F32)).astype(BF16)
            du_ref[rows, here] = (dh * by_up_ref[rows, units].astype(F32)).astype(BF16)
            score = score + jnp.sum(total * hidden_ref[rows, units].astype(F32), axis=1, keepdims=True)
        score = jnp.broadcast_to(score, (40, 256 - WIDTH))
        dx_ref[rows, WIDTH:] = score if before_ref is None else before_ref[rows, WIDTH:] + score
    copies = [pltpu.make_async_copy(dg_ref, dg_out, done.at[0]), pltpu.make_async_copy(du_ref, du_out, done.at[1])]
    for copy in copies:
        copy.start()
    units = pl.ds(pl.multiple_of(512 * half, 512), 512)
    dx = dot(dg_ref[...], wg_ref[:, units], OVER_UNITS) + dot(du_ref[...], wu_ref[:, units], OVER_UNITS)
    dx_ref[:, :WIDTH] = dx if before_ref is None else before_ref[:, :WIDTH] + dx
    return copies


def own_kernel(core_ref, *refs):
    for copy in half_grads(core_ref[0], *refs[:7], None, *refs[7:]):
        copy.wait()


def other_kernel(core_ref, *refs):
    given, dg_out, du_out, out_ref, back_ref, sent, dx_ref, scratch = refs[:8], *refs[8:14], refs[14:]
    copies = half_grads(1 - core_ref[0], *given, dg_out, du_out, dx_ref, *scratch)
    out, row = iota((8 * HOME, 8 * CAP), 0), iota((8 * HOME, 8 * CAP), 1)
    block, place = out // HOME, out % HOME
    same = row // CAP == block
    low = jnp.where(same & (row % CAP == place), 1.0, 0.0).astype(BF16)
    high = jnp.where(same & (row % CAP == place - CAP), 1.0, 0.0).astype(BF16)
    for j in range(4):
        rows = slice(8 * CAP * j, 8 * CAP * (j + 1))
        spread = dot(low, dx_ref[rows, :128].astype(BF16)) + dot(high, dx_ref[rows, 128:].astype(BF16))
        back_ref[8 * j : 8 * j + 8] = spread.astype(BF16).reshape(8, HOME, 128)
        quarter(back_ref, out_ref, sent, j).start()
    for copy in copies + [quarter(back_ref, out_ref, sent, j) for j in range(4)]:
        copy.wait()


def home_kernel(ids_ref, home_ref, tok_ref, gates_ref):
    ids = ids_ref[...]
    place, _ = places(ids, None)
    slot = iota((HOME, ROWS), 0).astype(F32)
    tables = [jnp.where(place[e : e + 1, :] == slot, 1.0, 0.0) for e in range(EXPERTS)]
    table = jnp.concatenate(tables, axis=0)
    past = jnp.where(place >= 0.0, place + CAP, -1.0)
    later = jnp.concatenate([jnp.where(past[e : e + 1, :] == slot, 1.0, 0.0) for e in range(EXPERTS)], axis=0)
    home = home_ref[...].reshape(EXPERTS * HOME, 128)
    tok_ref[:, :128] = dot(table.astype(BF16), home, OVER_ROWS).astype(BF16)
    tok_ref[:, 128:] = dot(later.astype(BF16), home, OVER_ROWS)[:, : WIDTH - 128].astype(BF16)
    score = home[:, WIDTH - 128 : WIDTH - 127].astype(F32)
    of_pair = jnp.sum((later * score).reshape(EXPERTS, HOME, ROWS), axis=1)
    expert = iota((EXPERTS, ROWS), 0)
    for k in range(TOP):
        hit = ids[k : k + 1, :] == expert
        gates_ref[k : k + 1, :] = jnp.sum(jnp.where(hit, of_pair, 0.0), axis=0, keepdims=True).astype(BF16)


def near(array):
    return pltpu.with_memory_space_constraint(array, pltpu.VMEM)


def call(body, outs, args, scratch=(), name=None, room=16):
    specs = [SMEM if a.dtype == jnp.int32 and a.ndim == 1 else VMEM for a in args]
    return pl.pallas_call(
        body,
        out_shape=[
            pltpu.VMEM(shape, dtype) if stays else jax.ShapeDtypeStruct(shape, dtype)
            for shape, dtype, stays in outs
        ],
        in_specs=specs,
        out_specs=[ANY if stays is None else VMEM for _, _, stays in outs],
        scratch_shapes=list(scratch),
        compiler_params=pltpu.CompilerParams(vmem_limit_bytes=room * 1024 * 1024),
        name=name,
    )(*args)


def on_device(tokens, cotangent, gates, expert_ids, saved_gate, saved_up, w_gate, w_up, w_down):
    ids = expert_ids.T
    core = lax.axis_index("tp_1").reshape(1)
    chips = lax.axis_size("tp_0")
    pairs = [(2 * z + c, 2 * z + 1 - c) for z in range(chips) for c in range(2)]
    send = call(
        pack_kernel, [((EXPERTS, PACK, 128), BF16, None)], [ids, gates.T, tokens, cotangent],
        [pltpu.VMEM((EXPERTS, PACK, 128), BF16), pltpu.SemaphoreType.DMA((4,))], name="pack", room=60,
    )[0]
    recv = lax.all_to_all(send, EP, 0, 0, tiled=True)
    units = ((SLOTS, UNITS), BF16, True)
    hidden, by_gate, by_up = call(
        factors_kernel,
        [units, units, units],
        [near(saved_gate[:, 0, :].T), near(saved_up[:, 0, :].T)],
        name="factors",
    )
    recv, hidden, by_gate, by_up = lax.optimization_barrier((recv, hidden, by_gate, by_up))
    half = ((chips, 40, 256), BF16, True)
    rows = ((SLOTS, WIDTH), BF16, True)
    down = near(w_down[0].T)
    given, dy, x, scaled, gate = call(
        product_kernel,
        [half, rows, ((SLOTS, WIDTH), BF16, False), rows, ((SLOTS, 128), F32, True)],
        [core, near(recv), down],
        name="product",
    )
    weights = ((WIDTH, UNITS), BF16, False)
    got = lax.ppermute(given, TP, pairs)
    kept, grad_w_down = call(
        kept_kernel, [half, weights], [core, near(dy), down, near(scaled), near(hidden)], name="kept"
    )
    got, kept = lax.optimization_barrier((got, kept))
    pair = call(pair_kernel, [half], [core, near(kept), near(got)], name="pair")[0]
    terms = lax.all_to_all(pair, "tp_0", 0, 0, tiled=True)

    copies = call(spread_kernel, [((chips, 40, 256), BF16, False)], [near(terms)], name="spread")[0]
    own = lax.all_to_all(copies, "tp_0", 0, 0, tiled=True)
    other = lax.ppermute(own, TP, pairs)
    wide_half = ((SLOTS, UNITS // 2), BF16, None)
    drafts = [pltpu.VMEM((SLOTS, UNITS // 2), BF16), pltpu.VMEM((SLOTS, UNITS // 2), BF16), pltpu.SemaphoreType.DMA((2,))]
    sums = ((SLOTS, 256), F32, True)
    shared = [near(gate), near(by_gate), near(by_up), near(hidden), near(w_gate[0]), near(w_up[0])]
    own_dg, own_du, own_dx = call(own_kernel, [wide_half, wide_half, sums], [core, near(own), *shared], drafts, name="own")
    other, own_dx = lax.optimization_barrier((other, own_dx))
    dg, du, back = call(
        other_kernel,
        [wide_half, wide_half, ((EXPERTS, HOME, 128), BF16, None)],
        [core, near(other), *shared, near(own_dx)],
        scratch=[
            pltpu.VMEM((EXPERTS, HOME, 128), BF16),
            pltpu.SemaphoreType.DMA((4,)),
            pltpu.VMEM((SLOTS, 256), F32),
            *drafts,
        ],
        name="other",
    )
    home = lax.all_to_all(back, EP, 0, 0, tiled=True)
    grad_w_gate, grad_w_up = call(
        weights_kernel,
        [weights, weights],
        [core, near(x), near(own_dg), near(own_du), near(dg), near(du)],
        name="weights",
    )
    grad_tokens, grad_gates = call(
        home_kernel, [((ROWS, WIDTH), BF16, False), ((TOP, ROWS), BF16, False)], [ids, near(home)], name="home"
    )
    return (grad_tokens, grad_gates.T, grad_w_gate[None], grad_w_up[None], grad_w_down.T[None])


def solution(mesh):
    split = Mesh(
        mesh.devices.reshape(mesh.shape["ex"], mesh.shape["ey"], mesh.shape["tp"] // 2, 2),
        ("ex", "ey", "tp_0", "tp_1"),
    )
    in_specs = (
        P(EP, TP),
        P(EP, TP),
        P(EP, None),
        P(EP, None),
        P(None, EP, None),
        P(None, EP, None),
        P(EP, TP, None),
        P(EP, TP, None),
        P(EP, None, TP),
    )
    out_specs = (
        P(EP, TP),
        P(EP, None),
        P(EP, TP, None),
        P(EP, TP, None),
        P(EP, None, TP),
    )
    return jax.shard_map(
        on_device, mesh=split, in_specs=in_specs, out_specs=out_specs, check_vma=False
    )
```

```python
import jax
import jax.numpy as jnp
from jax import lax
from jax.experimental import pallas as pl
from jax.experimental.pallas import tpu as pltpu
from jax.sharding import Mesh
from jax.sharding import PartitionSpec as P

EXPERTS = 32
TOP = 8
CAP = 10
ROWS = 32
WIDTH = 224
UNITS = 1024
SLOTS = 320
PACK = 40
HOME = 24
STAGGER = 6500
TP = ("tp_0", "tp_1")
EP = ("ex", "ey")
F32 = jnp.float32
BF16 = jnp.bfloat16
VMEM = pl.BlockSpec(memory_space=pltpu.VMEM)
SMEM = pl.BlockSpec(memory_space=pltpu.SMEM)
ANY = pl.BlockSpec(memory_space=pl.ANY)
OVER_UNITS = (((1,), (1,)), ((), ()))
OVER_ROWS = (((0,), (0,)), ((), ()))


def iota(shape, dim):
    return lax.broadcasted_iota(jnp.int32, shape, dim)


def dot(a, b, dims=(((1,), (0,)), ((), ()))):
    return lax.dot_general(a, b, dims, preferred_element_type=F32)


def places(ids, gates):
    expert = iota((EXPERTS, ROWS), 0)
    named = jnp.zeros((EXPERTS, ROWS), F32)
    weight = jnp.zeros((EXPERTS, ROWS), F32)
    for k in range(TOP):
        hit = ids[k : k + 1, :] == expert
        named = named + jnp.where(hit, 1.0, 0.0)
        if gates is not None:
            weight = weight + jnp.where(hit, gates[k : k + 1, :], 0.0)
    before = jnp.where(iota((ROWS, ROWS), 0) < iota((ROWS, ROWS), 1), 1.0, 0.0).astype(BF16)
    place = dot(named.astype(BF16), before)
    return jnp.where(named > 0.5, place, -1.0), weight


def quarter(block_ref, out_ref, done, j):
    rows = pl.ds(8 * j, 8)
    return pltpu.make_async_copy(block_ref.at[rows], out_ref.at[rows], done.at[j])


def pack_kernel(ids_ref, gates_ref, tok_ref, cot_ref, out_ref, block_ref, done):
    place, weight = places(ids_ref[...], gates_ref[...].astype(F32))
    place = jnp.concatenate([place] * 4, axis=1)
    weight = jnp.concatenate([weight] * 4, axis=1)
    row, lane = iota((PACK, 128), 0), iota((PACK, 128), 1)
    want = row - CAP * (lane // ROWS)
    want = jnp.where((want >= 0) & (want < CAP), want, -2).astype(F32)
    tail = lane >= 3 * ROWS
    tok, cot = tok_ref[...], cot_ref[...]
    zeros = jnp.zeros((ROWS, 64), BF16)
    source = jnp.concatenate(
        [
            tok[:, :128],
            cot[:, :128],
            jnp.concatenate([tok[:, 128:192], cot[:, 128:192]], axis=1),
            jnp.concatenate([tok[:, 192:224], cot[:, 192:224], zeros], axis=1),
        ],
        axis=0,
    )
    at_gate = jnp.where(iota((128, 128), 1) == 64, 1.0, 0.0).astype(BF16)
    source = jnp.concatenate([source, at_gate], axis=0)
    picks = []
    for e in range(EXPERTS):
        takes = place[e : e + 1, :] == want
        pick = jnp.where(takes, 1.0, 0.0)
        gate = jnp.where(takes & tail, weight[e : e + 1, :], 0.0)
        picks.append(jnp.concatenate([pick, gate], axis=1))
    for j in range(4):
        part = jnp.concatenate(picks[8 * j : 8 * j + 8], axis=0).astype(BF16)
        block_ref[8 * j : 8 * j + 8] = dot(part, source).astype(BF16).reshape(8, PACK, 128)
        quarter(block_ref, out_ref, done, j).start()
    for j in range(4):
        quarter(block_ref, out_ref, done, j).wait()


def half_product(dy, first, down_ref, out_ref):
    part = dot(dy, jnp.where(first, down_ref[:, :512], down_ref[:, 512:]))
    for v in range(2):
        for b in range(8):
            out_ref[8 * v + b] = part[40 * b : 40 * b + 40, 256 * v : 256 * v + 256].astype(BF16)


def kept_kernel(core_ref, dy_ref, down_ref, scaled_ref, hidden_ref, kept_ref, wd_ref):
    half_product(dy_ref[...], core_ref[0] == 0, down_ref, kept_ref)
    wd_ref[...] = dot(scaled_ref[...], hidden_ref[...], OVER_ROWS).astype(BF16)


def product_kernel(core_ref, recv_ref, down_ref, given_ref, dy_ref, x_ref, scaled_ref, gate_ref):
    to_x = jnp.concatenate([iota((128, 128), 1), iota((128, 128), 1)], axis=0)
    at = iota((256, 128), 0)
    from_x = jnp.where(to_x < 64, to_x, to_x + 64)
    from_x = jnp.where(to_x < 96, from_x, -1)
    from_dy = jnp.where(to_x < 64, to_x + 64, to_x + 96)
    from_dy = jnp.where(to_x < 96, from_dy, -1)
    x_move = jnp.where(at == from_x, 1.0, 0.0).astype(BF16)
    dy_move = jnp.where(at == from_dy, 1.0, 0.0).astype(BF16)
    slot, place = iota((8 * CAP, 8 * PACK), 0), iota((8 * CAP, 8 * PACK), 1)
    base = (slot // CAP) * PACK + slot % CAP
    picks = [jnp.where(place == base + CAP * kind, 1.0, 0.0).astype(BF16) for kind in range(4)]
    for j in range(4):
        got = recv_ref[8 * j : 8 * j + 8].reshape(8 * PACK, 128)
        x_low, dy_low, middle, last = [dot(pick, got) for pick in picks]
        tail = jnp.concatenate([middle, last], axis=1).astype(BF16)
        x_high = dot(tail, x_move)
        dy_high = dot(tail, dy_move)
        x = jnp.concatenate([x_low, x_high[:, :96]], axis=1)
        dy = jnp.concatenate([dy_low, dy_high[:, :96]], axis=1)
        gate = last[:, 64:65]
        rows = slice(8 * CAP * j, 8 * CAP * (j + 1))
        x_ref[rows, :] = x.astype(BF16)
        scaled_ref[rows, :] = (gate * dy).astype(BF16)
        gate_ref[rows, :] = jnp.broadcast_to(gate, (8 * CAP, 128))
        dy_ref[rows, :] = dy.astype(BF16)
    half_product(dy_ref[...], core_ref[0] == 1, down_ref, given_ref)


def factors_kernel(gate_ref, up_ref, hidden_ref, by_gate_ref, by_up_ref):
    for b in range(20):
        rows = slice(16 * b, 16 * b + 16)
        gate = gate_ref[rows, :].astype(F32)
        up = up_ref[rows, :].astype(F32)
        sigm = jax.nn.sigmoid(gate)
        by_up = gate * sigm
        hidden_ref[rows, :] = (by_up * up).astype(BF16)
        by_gate_ref[rows, :] = (up * sigm * (1.0 + gate * (1.0 - sigm))).astype(BF16)
        by_up_ref[rows, :] = by_up.astype(BF16)


def weights_kernel(core_ref, x_ref, own_dg_ref, own_du_ref, dg_ref, du_ref, wg_ref, wu_ref):
    core = core_ref[0]
    for half, dg, du in ((core, own_dg_ref, own_du_ref), (1 - core, dg_ref, du_ref)):
        units = pl.ds(pl.multiple_of(512 * half, 512), 512)
        wg_ref[:, units] = dot(x_ref[...], dg[...], OVER_ROWS).astype(BF16)
        wu_ref[:, units] = dot(x_ref[...], du[...], OVER_ROWS).astype(BF16)


def pair_kernel(core_ref, kept_ref, got_ref, pair_ref):
    @pl.when(core_ref[0] == 0)
    def _():
        pl.delay(STAGGER)

    for z in range(kept_ref.shape[0]):
        pair_ref[z] = (kept_ref[z].astype(F32) + got_ref[z].astype(F32)).astype(BF16)


def spread_kernel(terms_ref, copies_ref):
    total = terms_ref[0].astype(F32)
    for z in range(1, terms_ref.shape[0]):
        total = total + terms_ref[z].astype(F32)
    total = total.astype(BF16)
    for z in range(terms_ref.shape[0]):
        copies_ref[z] = total


def half_grads(half, half_ref, gate_ref, by_gate_ref, by_up_ref, hidden_ref, wg_ref, wu_ref, before_ref, dg_out, du_out, dx_ref, dg_ref, du_ref, done):
    for b in range(8):
        rows = slice(40 * b, 40 * b + 40)
        gate = gate_ref[rows, 0:1]
        score = jnp.zeros((40, 1), F32)
        for v in range(2):
            units = pl.ds(pl.multiple_of(512 * half + 256 * v, 256), 256)
            here = slice(256 * v, 256 * v + 256)
            total = half_ref[8 * v + b].astype(F32)
            dh = gate * total
            dg_ref[rows, here] = (dh * by_gate_ref[rows, units].astype(F32)).astype(BF16)
            du_ref[rows, here] = (dh * by_up_ref[rows, units].astype(F32)).astype(BF16)
            score = score + jnp.sum(total * hidden_ref[rows, units].astype(F32), axis=1, keepdims=True)
        score = jnp.broadcast_to(score, (40, 256 - WIDTH))
        dx_ref[rows, WIDTH:] = score if before_ref is None else before_ref[rows, WIDTH:] + score
    copies = [pltpu.make_async_copy(dg_ref, dg_out, done.at[0]), pltpu.make_async_copy(du_ref, du_out, done.at[1])]
    for copy in copies:
        copy.start()
    units = pl.ds(pl.multiple_of(512 * half, 512), 512)
    dx = dot(dg_ref[...], wg_ref[:, units], OVER_UNITS) + dot(du_ref[...], wu_ref[:, units], OVER_UNITS)
    dx_ref[:, :WIDTH] = dx if before_ref is None else before_ref[:, :WIDTH] + dx
    return copies


def own_kernel(core_ref, *refs):
    for copy in half_grads(core_ref[0], *refs[:7], None, *refs[7:]):
        copy.wait()


def other_kernel(core_ref, *refs):
    given, dg_out, du_out, out_ref, back_ref, sent, dx_ref, scratch = refs[:8], *refs[8:14], refs[14:]
    copies = half_grads(1 - core_ref[0], *given, dg_out, du_out, dx_ref, *scratch)
    out, row = iota((8 * HOME, 8 * CAP), 0), iota((8 * HOME, 8 * CAP), 1)
    block, place = out // HOME, out % HOME
    same = row // CAP == block
    low = jnp.where(same & (row % CAP == place), 1.0, 0.0).astype(BF16)
    high = jnp.where(same & (row % CAP == place - CAP), 1.0, 0.0).astype(BF16)
    for j in range(4):
        rows = slice(8 * CAP * j, 8 * CAP * (j + 1))
        spread = dot(low, dx_ref[rows, :128].astype(BF16)) + dot(high, dx_ref[rows, 128:].astype(BF16))
        back_ref[8 * j : 8 * j + 8] = spread.astype(BF16).reshape(8, HOME, 128)
        quarter(back_ref, out_ref, sent, j).start()
    for copy in copies + [quarter(back_ref, out_ref, sent, j) for j in range(4)]:
        copy.wait()


def home_kernel(ids_ref, home_ref, tok_ref, gates_ref):
    ids = ids_ref[...]
    place, _ = places(ids, None)
    slot = iota((HOME, ROWS), 0).astype(F32)
    tables = [jnp.where(place[e : e + 1, :] == slot, 1.0, 0.0) for e in range(EXPERTS)]
    table = jnp.concatenate(tables, axis=0)
    past = jnp.where(place >= 0.0, place + CAP, -1.0)
    later = jnp.concatenate([jnp.where(past[e : e + 1, :] == slot, 1.0, 0.0) for e in range(EXPERTS)], axis=0)
    home = home_ref[...].reshape(EXPERTS * HOME, 128)
    tok_ref[:, :128] = dot(table.astype(BF16), home, OVER_ROWS).astype(BF16)
    tok_ref[:, 128:] = dot(later.astype(BF16), home, OVER_ROWS)[:, : WIDTH - 128].astype(BF16)
    score = home[:, WIDTH - 128 : WIDTH - 127].astype(F32)
    of_pair = jnp.sum((later * score).reshape(EXPERTS, HOME, ROWS), axis=1)
    expert = iota((EXPERTS, ROWS), 0)
    for k in range(TOP):
        hit = ids[k : k + 1, :] == expert
        gates_ref[k : k + 1, :] = jnp.sum(jnp.where(hit, of_pair, 0.0), axis=0, keepdims=True).astype(BF16)


def near(array):
    return pltpu.with_memory_space_constraint(array, pltpu.VMEM)


def call(body, outs, args, scratch=(), name=None, room=16):
    specs = [SMEM if a.dtype == jnp.int32 and a.ndim == 1 else VMEM for a in args]
    return pl.pallas_call(
        body,
        out_shape=[
            pltpu.VMEM(shape, dtype) if stays else jax.ShapeDtypeStruct(shape, dtype)
            for shape, dtype, stays in outs
        ],
        in_specs=specs,
        out_specs=[ANY if stays is None else VMEM for _, _, stays in outs],
        scratch_shapes=list(scratch),
        compiler_params=pltpu.CompilerParams(vmem_limit_bytes=room * 1024 * 1024),
        name=name,
    )(*args)


def on_device(tokens, cotangent, gates, expert_ids, saved_gate, saved_up, w_gate, w_up, w_down):
    ids = expert_ids.T
    core = lax.axis_index("tp_1").reshape(1)
    chips = lax.axis_size("tp_0")
    pairs = [(2 * z + c, 2 * z + 1 - c) for z in range(chips) for c in range(2)]
    send = call(
        pack_kernel, [((EXPERTS, PACK, 128), BF16, None)], [ids, gates.T, tokens, cotangent],
        [pltpu.VMEM((EXPERTS, PACK, 128), BF16), pltpu.SemaphoreType.DMA((4,))], name="pack", room=60,
    )[0]
    recv = lax.all_to_all(send, EP, 0, 0, tiled=True)
    units = ((SLOTS, UNITS), BF16, True)
    hidden, by_gate, by_up = call(
        factors_kernel,
        [units, units, units],
        [near(saved_gate[:, 0, :].T), near(saved_up[:, 0, :].T)],
        name="factors",
    )
    recv, hidden, by_gate, by_up = lax.optimization_barrier((recv, hidden, by_gate, by_up))
    half = ((chips, 40, 256), BF16, True)
    rows = ((SLOTS, WIDTH), BF16, True)
    down = near(w_down[0].T)
    given, dy, x, scaled, gate = call(
        product_kernel,
        [half, rows, ((SLOTS, WIDTH), BF16, False), rows, ((SLOTS, 128), F32, True)],
        [core, near(recv), down],
        name="product",
    )
    weights = ((WIDTH, UNITS), BF16, False)
    got = lax.ppermute(given, TP, pairs)
    kept, grad_w_down = call(
        kept_kernel, [half, weights], [core, near(dy), down, near(scaled), near(hidden)], name="kept"
    )
    got, kept = lax.optimization_barrier((got, kept))
    pair = call(pair_kernel, [half], [core, near(kept), near(got)], name="pair")[0]
    terms = lax.all_to_all(pair, "tp_0", 0, 0, tiled=True)

    copies = call(spread_kernel, [((chips, 40, 256), BF16, False)], [near(terms)], name="spread")[0]
    own = lax.all_to_all(copies, "tp_0", 0, 0, tiled=True)
    other = lax.ppermute(own, TP, pairs)
    wide_half = ((SLOTS, UNITS // 2), BF16, None)
    drafts = [pltpu.VMEM((SLOTS, UNITS // 2), BF16), pltpu.VMEM((SLOTS, UNITS // 2), BF16), pltpu.SemaphoreType.DMA((2,))]
    sums = ((SLOTS, 256), F32, True)
    shared = [near(gate), near(by_gate), near(by_up), near(hidden), near(w_gate[0]), near(w_up[0])]
    own_dg, own_du, own_dx = call(own_kernel, [wide_half, wide_half, sums], [core, near(own), *shared], drafts, name="own")
    other, own_dx = lax.optimization_barrier((other, own_dx))
    dg, du, back = call(
        other_kernel,
        [wide_half, wide_half, ((EXPERTS, HOME, 128), BF16, None)],
        [core, near(other), *shared, near(own_dx)],
        scratch=[
            pltpu.VMEM((EXPERTS, HOME, 128), BF16),
            pltpu.SemaphoreType.DMA((4,)),
            pltpu.VMEM((SLOTS, 256), F32),
            *drafts,
        ],
        name="other",
    )
    home = lax.all_to_all(back, EP, 0, 0, tiled=True)
    grad_w_gate, grad_w_up = call(
        weights_kernel,
        [weights, weights],
        [core, near(x), near(own_dg), near(own_du), near(dg), near(du)],
        name="weights",
    )
    grad_tokens, grad_gates = call(
        home_kernel, [((ROWS, WIDTH), BF16, False), ((TOP, ROWS), BF16, False)], [ids, near(home)], name="home"
    )
    return (grad_tokens, grad_gates.T, grad_w_gate[None], grad_w_up[None], grad_w_down.T[None])


def solution(mesh):
    split = Mesh(
        mesh.devices.reshape(mesh.shape["ex"], mesh.shape["ey"], mesh.shape["tp"] // 2, 2),
        ("ex", "ey", "tp_0", "tp_1"),
    )
    in_specs = (
        P(EP, TP),
        P(EP, TP),
        P(EP, None),
        P(EP, None),
        P(None, EP, None),
        P(None, EP, None),
        P(EP, TP, None),
        P(EP, TP, None),
        P(EP, None, TP),
    )
    out_specs = (
        P(EP, TP),
        P(EP, None),
        P(EP, TP, None),
        P(EP, TP, None),
        P(EP, None, TP),
    )
    return jax.shard_map(
        on_device, mesh=split, in_specs=in_specs, out_specs=out_specs, check_vma=False
    )
```
